128 devices in a mesh: dp: 4 (over x), vocab: 32 (over y, z, core).
Axes of the slice: x: 4, y: 4, z: 4, core: 2. Of those that a mesh axis runs over, the one named last changes fastest.
Arguments:
- hidden: bfloat16 [1024, 5120], P('dp')
- head_t: bfloat16 [5120, 77824], P('dp', 'vocab'), may hold values from -0.25 to 0.25
- targets: int32 [1024], P('dp'), may hold values from 0 to 77823
- token_ids: int32 [1024], P('dp'), may hold values from 0 to 77823, as said below
- embed_cot: bfloat16 [1024, 5120], P('dp'), may hold values from -6 to 6
Outputs:
- head_grad: bfloat16 [5120, 77824], P('dp', 'vocab')
- embed_grad: bfloat16 [5120, 77824], P('dp', 'vocab')
- hidden_grad: bfloat16 [1024, 5120], P('vocab', 'dp')
The draws below stay inside these ranges and needn't reach their ends.
Inputs may be any that keep to these rules, and one draw needn't show every extreme that they name: `token_ids`: among the 256 input ids of one data group, at most 16 lie in any one block of 2432 vocabulary rows that starts at a multiple of 2432; in every group some block holds exactly 16.
All inputs are finite; a program needn't handle non-finite values.
Results may differ from the reference program's by a relative error of at most 0.0033.
Values may be sent and summed in bfloat16 or wider, within the bound.
No kernel may reach another device: no remote copies, remote signals or barrier semaphores. Data moves between devices by JAX's collectives and lax.ppermute only.
A program may use at most 128 MiB of HBM per device.

```python
import math
import jax
import jax.numpy as jnp
import numpy as np

D = 5120
V_DEV = 2432
TOK_DEV = 256
VOCAB = 77824
TOKENS = 1024


def draw_hidden(key, part):
    base_key = jax.random.fold_in(key, 11)
    values = jax.random.normal(base_key, (TOKENS, D), jnp.float32)
    strong_rows = jax.random.randint(jax.random.fold_in(key, 13), (4,), 0, TOKENS)
    strengths = jnp.array([20.0, 30.0, 40.0, 45.0], jnp.float32)
    row_numbers = jnp.arange(TOKENS, dtype=jnp.int32)
    boost = jnp.ones((TOKENS,), jnp.float32)
    boost = jnp.where(row_numbers == strong_rows[0], strengths[0], boost)
    boost = jnp.where(row_numbers == strong_rows[1], strengths[1], boost)
    boost = jnp.where(row_numbers == strong_rows[2], strengths[2], boost)
    boost = jnp.where(row_numbers == strong_rows[3], strengths[3], boost)
    values = values * boost[:, None]
    return values.astype(jnp.bfloat16)


def group_ids(group_key):
    blocks = VOCAB // V_DEV
    bound = 2 * TOK_DEV // blocks
    slots = bound * blocks
    full_block = jax.random.randint(jax.random.fold_in(group_key, 1), (), 0, blocks)
    priority = jax.random.permutation(jax.random.fold_in(group_key, 2), slots).astype(jnp.int32)
    slot_block = jnp.arange(slots, dtype=jnp.int32) // bound
    priority = jnp.where(slot_block == full_block, -1, priority)
    chosen = jnp.argsort(priority, stable=True)[:TOK_DEV].astype(jnp.int32) // bound
    shuffled = jax.random.permutation(jax.random.fold_in(group_key, 3), chosen)
    offsets = jax.random.randint(jax.random.fold_in(group_key, 4), (TOK_DEV,), 0, V_DEV)
    return (shuffled * V_DEV + offsets).astype(jnp.int32)


def draw_token_ids(key, part):
    group_count = TOKENS // TOK_DEV
    numbers = jnp.arange(group_count, dtype=jnp.int32)
    keys = jax.vmap(lambda number: jax.random.fold_in(key, 31 + number))(numbers)
    return jax.vmap(group_ids)(keys).reshape(TOKENS)


def set_ends(result, stream_key, smallest, high):
    longest = result.shape.index(max(result.shape))
    spots = []
    for shift in (0, 1):
        where = [jax.random.randint(jax.random.fold_in(stream_key, axis), (), 0, length) for axis, length in enumerate(result.shape)]
        where[longest] = (where[longest] + shift) % result.shape[longest]
        spots.append(tuple(where))
    return result.at[spots[0]].set(smallest).at[spots[1]].set(high)


def levels(key, shape, split, least, top_value):
    gain, own = 1.0, jax.random.fold_in(key, 6)
    for position, blocks in split:
        heights = jnp.exp(jax.random.uniform(jax.random.fold_in(own, position), (blocks,), jnp.float32, least / len(split), top_value / len(split)))
        gain = gain * jnp.repeat(heights, shape[position] // blocks).reshape([-1 if axis == position else 1 for axis in range(len(shape))])
    return gain


def ranked_wide(rng, extent, count, skew):
    portions = [min(1 << octave, count + 1 - (1 << octave)) * (1 << 20) // math.isqrt((1 << octave) ** skew) + 1 for octave in range((count + 1).bit_length()) if 1 << octave <= count]
    width = 1 + sum(portions) // (1 << 30)
    grid = np.cumsum(np.array([max(1, weight // width) for weight in portions]))
    ticket = jax.random.randint(jax.random.fold_in(rng, 1), extent, 0, int(grid[len(portions) - 1]))
    start = jnp.left_shift(1, jnp.searchsorted(jnp.asarray(grid, jnp.int32), ticket, side="right").astype(jnp.int32))
    grade = start - 1 + jax.random.randint(jax.random.fold_in(rng, 4), extent, 0, 1 << 30) % jnp.minimum(start, count + 1 - start)
    return jax.random.permutation(jax.random.fold_in(rng, 2), count)[grade].astype(jnp.int32)


def bell_draw(stream_key, extent, width, reach, pieces=(), held_as=jnp.bfloat16):
    loudness = levels(stream_key, extent, pieces, -0.22, 0.18) if pieces else 1.0
    values = jax.random.normal(stream_key, extent, jnp.float32) * width * loudness
    return jnp.minimum(jnp.maximum(values, -reach), reach).astype(held_as)


def setup_inputs(seed: int = 0) -> dict:
    key_of = jax.random.split(jax.random.key(seed), 6)
    hidden = draw_hidden(jax.random.fold_in(key_of[5], 71), 0)
    head_t = bell_draw(key_of[1], (D, VOCAB), (D // 9) ** -0.5, 0.25, ((0, 4), (1, 32)))
    targets = set_ends(ranked_wide(key_of[2], (TOKENS,), VOCAB, 1), jax.random.fold_in(key_of[2], 3), 0, VOCAB - 1).astype(jnp.int32)
    token_ids = draw_token_ids(jax.random.fold_in(key_of[5], 71), 0)
    embed_cot = bell_draw(key_of[4], (TOKENS, D), 1.0, 6.0, ((0, 4),))
    return dict(hidden=hidden, head_t=head_t, targets=targets, token_ids=token_ids, embed_cot=embed_cot)


def reference(hidden, head_t, targets, token_ids, embed_cot):
    logits = jnp.dot(hidden, head_t, preferred_element_type=jnp.float32)
    row_max = jnp.max(logits, axis=1, keepdims=True)
    expo = jnp.exp(logits - row_max)
    row_sum = jnp.sum(expo, axis=1, keepdims=True)
    columns = jnp.arange(VOCAB, dtype=jnp.int32)[None, :]
    target_hot = (columns == targets[:, None]).astype(jnp.float32)
    dlogits = (expo / row_sum - target_hot).astype(jnp.bfloat16)
    head_grad = jnp.dot(hidden.T, dlogits, preferred_element_type=jnp.float32).astype(jnp.bfloat16)
    hidden_grad = jnp.dot(dlogits, head_t.T, preferred_element_type=jnp.float32).astype(jnp.bfloat16)
    id_hot = (columns == token_ids[:, None]).astype(jnp.bfloat16)
    embed_grad = jnp.dot(embed_cot.T, id_hot, preferred_element_type=jnp.float32).astype(jnp.bfloat16)
    return head_grad, embed_grad, hidden_grad
```

```python
import functools

import jax
import jax.numpy as jnp
from jax import lax
from jax.experimental import pallas as pl
from jax.experimental.pallas import tpu as pltpu
from jax.sharding import PartitionSpec as P


LANES = 128
BF = jnp.bfloat16
F32 = jnp.float32


def wire(x):
    return lax.optimization_barrier(x)


def shift_x(a, s):
    n = lax.axis_size("dp")
    return lax.ppermute(a, "dp", [(i, (i + s) % n) for i in range(n)])


def vocab_perm(dy, dz, dc):
    pairs = []
    for v in range(32):
        y, z, c = v // 8, (v // 2) % 4, v % 2
        pairs.append((v, ((y + dy) % 4) * 8 + ((z + dz) % 4) * 2 + (c + dc) % 2))
    return pairs


def shift_v(a, dy, dz, dc):
    return lax.ppermute(a, "vocab", vocab_perm(dy, dz, dc))


def pack_kernel(offs, *refs):
    n = len(refs) // 2
    for src, dst in zip(refs[:n], refs[n:]):
        dst[...] = src[...]


def pack(head_t, offs, tiles):
    rows, n = head_t.shape[0], offs.shape[0]

    def at(s):
        return lambda t, o: (0, o[s] + t)

    return pl.pallas_call(
        pack_kernel,
        grid_spec=pltpu.PrefetchScalarGridSpec(
            num_scalar_prefetch=1,
            grid=(tiles,),
            in_specs=[pl.BlockSpec((rows, LANES), at(s)) for s in range(n)],
            out_specs=[pl.BlockSpec((rows, LANES), lambda t, o: (0, t))] * n,
        ),
        out_shape=[jax.ShapeDtypeStruct((rows, tiles * LANES), BF)] * n,
        name="pack",
    )(offs, *([head_t] * n))


def first_kernel(q, ha, hb, wa, wb, out):
    out[...] = jnp.dot(ha[...], wa[...], preferred_element_type=F32) + jnp.dot(
        hb[...], wb[...], preferred_element_type=F32
    )


def logits_first(hid, q, wa, wb, block):
    depth, width = wa.shape
    rows = hid.shape[0]
    return pl.pallas_call(
        first_kernel,
        grid_spec=pltpu.PrefetchScalarGridSpec(
            num_scalar_prefetch=1,
            grid=(rows // block,),
            in_specs=[
                pl.BlockSpec((block, depth), lambda t, q: (t, q[0])),
                pl.BlockSpec((block, depth), lambda t, q: (t, q[1])),
                pl.BlockSpec((depth, width), lambda t, q: (0, 0)),
                pl.BlockSpec((depth, width), lambda t, q: (0, 0)),
            ],
            out_specs=pl.BlockSpec((block, width), lambda t, q: (t, 0)),
        ),
        out_shape=jax.ShapeDtypeStruct((rows, width), F32),
        cost_estimate=pl.CostEstimate(
            flops=4 * rows * depth * width, bytes_accessed=12_000_000, transcendentals=0
        ),
        name="logits_first",
    )(q, hid, hid, wa, wb)


def last_kernel(q, hc, hd, wc, wd, acc, tgt, e_out, st_out):
    logits = acc[...] + (
        jnp.dot(hc[...], wc[...], preferred_element_type=F32)
        + jnp.dot(hd[...], wd[...], preferred_element_type=F32)
    )
    top = jnp.max(logits, axis=1, keepdims=True)
    expo = jnp.exp(logits - top)
    col = lax.broadcasted_iota(jnp.int32, logits.shape, 1)
    mine = col < q[2]
    total = jnp.sum(jnp.where(mine, expo, 0.0), axis=1, keepdims=True)
    hit = (col == tgt[...]) & mine
    at_target = jnp.sum(jnp.where(hit, logits, 0.0), axis=1, keepdims=True)
    e_out[...] = expo.astype(BF)
    lane = lax.broadcasted_iota(jnp.int32, st_out.shape, 1)
    st_out[...] = jnp.where(lane == 0, top, jnp.where(lane == 1, total, at_target))


def logits_last(hid, q, wc, wd, acc, tgt, start, rows, block):
    depth, width = wc.shape
    first = start // block
    return pl.pallas_call(
        last_kernel,
        grid_spec=pltpu.PrefetchScalarGridSpec(
            num_scalar_prefetch=1,
            grid=(rows // block,),
            in_specs=[
                pl.BlockSpec((block, depth), lambda t, q: (t + first, q[0])),
                pl.BlockSpec((block, depth), lambda t, q: (t + first, q[1])),
                pl.BlockSpec((depth, width), lambda t, q: (0, 0)),
                pl.BlockSpec((depth, width), lambda t, q: (0, 0)),
                pl.BlockSpec((block, width), lambda t, q: (t + first, 0)),
                pl.BlockSpec((block, 1), lambda t, q: (t + first, 0)),
            ],
            out_specs=[
                pl.BlockSpec((block, width), lambda t, q: (t, 0)),
                pl.BlockSpec((block, LANES), lambda t, q: (t, 0)),
            ],
        ),
        out_shape=[
            jax.ShapeDtypeStruct((rows, width), BF),
            jax.ShapeDtypeStruct((rows, LANES), F32),
        ],
        cost_estimate=pl.CostEstimate(
            flops=4 * rows * depth * width, bytes_accessed=10_000_000, transcendentals=0
        ),
        name="logits_last",
    )(q, hid, hid, wc, wd, acc, tgt)


def dlogits_kernel(offs, e0, e1, e2, e3, coef, tgt, out):
    for s, e in enumerate((e0, e1, e2, e3)):
        start = pl.multiple_of(offs[s] * LANES, LANES)
        col = lax.broadcasted_iota(jnp.int32, e.shape, 1) + start
        prob = e[...].astype(F32) * coef[:, s : s + 1]
        grad = jnp.where(col == tgt[...], coef[:, 4:5], prob)
        out[:, pl.ds(start, e.shape[1])] = grad.astype(BF)


def dlogits_of(offs, es, coef, tgt, width_dev, start, block):
    rows, width = es[0].shape
    first = start // block
    return pl.pallas_call(
        dlogits_kernel,
        grid_spec=pltpu.PrefetchScalarGridSpec(
            num_scalar_prefetch=1,
            grid=(rows // block,),
            in_specs=[pl.BlockSpec((block, width), lambda t, o: (t, 0))] * 4
            + [
                pl.BlockSpec((block, LANES), lambda t, o: (t + first, 0)),
                pl.BlockSpec((block, 1), lambda t, o: (t + first, 0)),
            ],
            out_specs=pl.BlockSpec((block, width_dev), lambda t, o: (t, 0)),
        ),
        out_shape=jax.ShapeDtypeStruct((rows, width_dev), BF),
        cost_estimate=pl.CostEstimate(
            flops=8_000_000, bytes_accessed=8 * rows * width_dev, transcendentals=0
        ),
        name="dlogits",
    )(offs, *es, coef, tgt)


def head_kernel(ht, *refs):
    grads, out = refs[:-1], refs[-1]
    total = None
    at = 0
    for g in grads:
        depth = g.shape[0]
        part = jnp.dot(ht[:, at : at + depth], g[...], preferred_element_type=F32)
        total = part if total is None else total + part
        at += depth
    out[...] = total.astype(BF)


def head_grad_of(ht, grads, block):
    rows, depth = ht.shape
    width = grads[0].shape[1]
    return pl.pallas_call(
        head_kernel,
        grid=(rows // block,),
        in_specs=[pl.BlockSpec((block, depth), lambda i: (i, 0))]
        + [pl.BlockSpec(g.shape, lambda i: (0, 0)) for g in grads],
        out_specs=pl.BlockSpec((block, width), lambda i: (i, 0)),
        out_shape=jax.ShapeDtypeStruct((rows, width), BF),
        cost_estimate=pl.CostEstimate(
            flops=2 * rows * depth * width, bytes_accessed=16_000_000, transcendentals=0
        ),
        name="head_grad",
    )(ht, *grads)


def from_planes(own, next_, across, prev, x):
    return jnp.roll(jnp.stack([own, next_, across, prev]), x, axis=0)


def everywhere(a):
    return a, shift_x(a, -1), shift_x(a, 2), shift_x(a, 1)


def scatter_tokens(part, y, z, c):
    depth = part.shape[-1]
    half = depth // 2
    part = part.reshape(-1, 4, 2, 4, 8, depth)
    pick = lambda a, i, axis: lax.dynamic_index_in_dim(a, i, axis, keepdims=False)
    mine = pick(part, c, 2) + shift_v(pick(part, 1 - c, 2), 0, 0, 1)

    def along_y(a, axis):
        got = [shift_v(pick(a, (y + s) % 4, axis), s, 0, 0) for s in (1, 3, 2)]
        return pick(a, y, axis) + got[0] + got[1] + got[2]

    def along_z(a, axis):
        got = [shift_v(pick(a, (z + s) % 4, axis), 0, s, 0) for s in (1, 3, 2)]
        return pick(a, z, axis) + got[0] + got[1] + got[2]

    left, right = mine[..., :half], mine[..., half:]
    left, right = along_y(left, 2), along_z(right, 1)
    left, right = along_z(left, 1), along_y(right, 1)
    out = jnp.concatenate([left, right], axis=-1)
    return out.reshape(-1, depth)


def on_device(hidden, head_t, targets, token_ids, embed_cot):
    x, v = lax.axis_index("dp"), lax.axis_index("vocab")
    y, z, c = v // 8, (v // 2) % 4, v % 2
    depth, width_dev = head_t.shape
    group = hidden.shape[0]
    planes = lax.axis_size("dp")
    tokens = group * planes
    tiles_dev = width_dev // LANES
    tiles = -(-tiles_dev // planes)
    width = tiles * LANES
    base = v * width_dev
    chunks = 2
    rows = tokens // chunks

    def off(q):
        return jnp.minimum(q * tiles, tiles_dev - tiles)

    slot_plane = [(x + s) % planes for s in range(planes)]
    offs = jnp.stack([off(q) for q in slot_plane]).astype(jnp.int32)

    k, w = v // 8, v % 8
    rows_mine = lax.dynamic_slice_in_dim(hidden, 32 * w + 8 * k, 8, axis=0)
    ints = jnp.stack([targets, token_ids]).reshape(4, LANES)
    row_parts = everywhere(rows_mine)
    int_parts = everywhere(ints)
    own_w, to_next, to_across, to_prev = pack(head_t, offs, tiles)
    w_prev = shift_x(to_next, 1)
    w_next = shift_x(to_prev, -1)
    w_across = shift_x(to_across, 2)
    thirty_two = from_planes(*row_parts, x).reshape(-1, hidden.shape[1])
    hid = lax.all_gather(thirty_two, "vocab", axis=0, tiled=True)

    int_parts = [p.reshape(2, group) for p in int_parts]
    tgt = from_planes(*[p[0] for p in int_parts], x)
    tgt = tgt.reshape(4, 8, 4, 8).transpose(2, 1, 0, 3).reshape(tokens, 1) - base

    bound = 2 * group // lax.axis_size("vocab")
    slot_numbers = jnp.arange(bound, dtype=jnp.int32)

    def compact(ids):
        inside = (ids >= base) & (ids < base + width_dev)
        rank = jnp.cumsum(inside.astype(jnp.int32)) - 1
        return (rank[None, :] == slot_numbers[:, None]) & inside[None, :]

    group_ids = jnp.stack([p[1] for p in int_parts])
    matches = jax.vmap(compact)(group_ids)
    picked = jnp.dot(
        matches[0].astype(BF), embed_cot, preferred_element_type=F32
    ).astype(BF)

    def cot_for(s):
        return lax.dynamic_slice_in_dim(picked, slot_plane[s] * depth, depth, axis=1)

    received = jnp.concatenate(
        [cot_for(0), shift_x(cot_for(3), -1), shift_x(cot_for(2), 2), shift_x(cot_for(1), 1)]
    )
    slot_ids = jnp.sum(jnp.where(matches, group_ids[:, None, :] - base, 0), axis=-1)
    slot_ids = jnp.where(jnp.any(matches, axis=-1), slot_ids, -1).reshape(-1)
    local_columns = jnp.arange(width_dev, dtype=jnp.int32)[None, :]
    slot_hot = (local_columns == slot_ids[:, None]).astype(BF)
    embed_grad = lax.dot_general(
        received, slot_hot, (((0,), (0,)), ((), ())), preferred_element_type=F32
    ).astype(BF)

    valid = jnp.where(x == planes - 2, (tiles_dev - tiles - off(x)) * LANES, width)
    q_first = jnp.stack([slot_plane[0], slot_plane[3]]).astype(jnp.int32)
    q_last = jnp.stack([slot_plane[1], slot_plane[2], valid]).astype(jnp.int32)
    acc = logits_first(hid, q_first, own_w, w_prev, 256)
    tgt_own = tgt - off(x) * LANES
    expo, stats = [], []
    for i in range(chunks):
        e, st = logits_last(hid, q_last, w_next, w_across, acc, tgt_own, i * rows, rows, 256)
        expo.append(e)
        stats.append(st)

    es = []
    for e in expo:
        half = rows // 2
        prev, next_ = shift_x(e, 1), shift_x(e, -1)
        top = shift_x(prev[:half], 1)
        low = shift_x(next_[half:], -1)
        es.append((e, next_, jnp.concatenate([top, low]), prev))

    st = jnp.concatenate(stats)[:, :3].T.reshape(3, tokens // LANES, LANES)
    both = jnp.broadcast_to(st, (lax.axis_size("vocab"), *st.shape))
    both = lax.all_to_all(both, "vocab", split_axis=0, concat_axis=0, tiled=True)

    def joined(tops, sums, hits):
        top = jnp.max(tops, axis=0)
        return top, jnp.sum(sums * jnp.exp(tops - top), axis=0), jnp.sum(hits, axis=0)

    plane_stats = jnp.stack([*joined(both[:, 0], both[:, 1], both[:, 2]), st[0]])
    parts = jnp.stack(everywhere(plane_stats))
    row_max, row_sum, hit = joined(parts[:, 0], parts[:, 1], parts[:, 2])
    scale = jnp.exp(parts[:, 3] - row_max) / row_sum
    at_target = jnp.exp(hit - row_max) / row_sum - 1.0
    coef = jnp.concatenate([scale, at_target[None]]).reshape(5, tokens).T
    coef = jnp.pad(coef, ((0, 0), (0, LANES - 5)))

    grads, pieces = [], []
    for i in range(chunks):
        g = dlogits_of(offs, es[i], coef, tgt, width_dev, i * rows, 256)
        grads.append(g)
        part = lax.dot_general(g, head_t, (((1,), (1,)), ((), ())), preferred_element_type=F32)
        pieces.append(scatter_tokens(part, y, z, c))
    hidden_grad = jnp.concatenate(pieces).astype(BF)

    hid_own = lax.dynamic_slice_in_dim(hid, x * depth, depth, axis=1).T
    head_grad = head_grad_of(hid_own, grads, 256)
    return (head_grad, embed_grad, hidden_grad)


def solution(mesh):
    placed = (P("dp", None), P("dp", "vocab"), P("dp"), P("dp"), P("dp", None))
    return jax.shard_map(
        on_device,
        mesh=mesh,
        in_specs=placed,
        out_specs=(P("dp", "vocab"), P("dp", "vocab"), P("vocab", "dp")),
        check_vma=False,
    )
```

```python
import jax
import jax.numpy as jnp
from jax import lax
from jax.experimental import pallas as pl
from jax.experimental.pallas import tpu as pltpu
from jax.sharding import PartitionSpec as P


LANES = 128
BF = jnp.bfloat16
F32 = jnp.float32


def shift_x(a, s):
    n = lax.axis_size("dp")
    return lax.ppermute(a, "dp", [(i, (i + s) % n) for i in range(n)])


def vocab_perm(dy, dz, dc):
    pairs = []
    for v in range(32):
        y, z, c = v // 8, (v // 2) % 4, v % 2
        pairs.append((v, ((y + dy) % 4) * 8 + ((z + dz) % 4) * 2 + (c + dc) % 2))
    return pairs


def shift_v(a, dy, dz, dc):
    return lax.ppermute(a, "vocab", vocab_perm(dy, dz, dc))


def vmem(mib):
    return pltpu.CompilerParams(vmem_limit_bytes=mib * 2**20)


def pack_kernel(offs, *refs):
    n = len(refs) // 2
    for src, dst in zip(refs[:n], refs[n:]):
        dst[...] = src[...]


def pack(head_t, offs, tiles):
    rows, n = head_t.shape[0], offs.shape[0]

    def at(s):
        return lambda t, o: (0, o[s] + t)

    return pl.pallas_call(
        pack_kernel,
        grid_spec=pltpu.PrefetchScalarGridSpec(
            num_scalar_prefetch=1,
            grid=(tiles,),
            in_specs=[pl.BlockSpec((rows, LANES), at(s)) for s in range(n)],
            out_specs=[pl.BlockSpec((rows, LANES), lambda t, o: (0, t))] * n,
        ),
        out_shape=[jax.ShapeDtypeStruct((rows, tiles * LANES), BF)] * n,
        compiler_params=vmem(6),
        name="pack",
    )(offs, *([head_t] * n))


def assemble_kernel(at, p0, p1, p2, p3, left, right):
    depth = left.shape[-1] // 2
    for s, p in enumerate((p0, p1, p2, p3)):
        j = at[s]
        for dst, first, second in ((left, 0, 3), (right, 1, 2)):
            for i, slot in enumerate((first, second)):
                start = pl.multiple_of(at[slot] * depth, depth)
                dst[j, :, i * depth : (i + 1) * depth] = p[:, pl.ds(start, depth)]
        right[j, :, 2 * depth :] = p[:, 4 * depth :]


def assemble(at, parts, depth):
    rows = parts[0].shape[0]
    whole = lambda shape: pl.BlockSpec(shape, lambda i, at: (0,) * len(shape))
    shapes = [(4, rows, 2 * depth), (4, rows, 2 * depth + LANES)]
    return pl.pallas_call(
        assemble_kernel,
        grid_spec=pltpu.PrefetchScalarGridSpec(
            num_scalar_prefetch=1,
            grid=(1,),
            in_specs=[whole(parts[0].shape)] * 4,
            out_specs=[whole(s) for s in shapes],
        ),
        out_shape=[jax.ShapeDtypeStruct(s, BF) for s in shapes],
        compiler_params=vmem(8),
        name="assemble",
    )(at, *parts)


def add_products(total, pairs, weights):
    half = pairs[0][0].shape[0]
    for i in range(2):
        part = None
        for pair, w in zip(pairs, weights):
            new = jnp.dot(pair[i][...], w[...], preferred_element_type=F32)
            part = new if part is None else part + new
        total[i * half : (i + 1) * half, :] += part


def first_kernel(own1, oth1, own2, oth2, w1, w2, out):
    @pl.when(pl.program_id(0) == 0)
    def _():
        out[...] = jnp.zeros_like(out)

    add_products(out, ((own1, oth1), (own2, oth2)), (w1, w2))


def mid_kernel(own, oth, w, acc, out):
    @pl.when(pl.program_id(0) == 0)
    def _():
        out[...] = acc[...]

    add_products(out, ((own, oth),), (w,))


def strips(half, step, start):
    spec = lambda: pl.BlockSpec((half, step), lambda t, *q: (0, t + start))
    return [spec(), spec()]


def partial_logits(kernel, sources, weights, acc, step):
    depth, width = weights[0].shape
    steps = depth // step
    half = sources[0][0].shape[0]
    specs, args = [], []
    for own, oth, start in sources:
        specs += strips(half, step, start * steps)
        args += [own, oth]
    specs += [pl.BlockSpec((step, width), lambda t: (t, 0))] * len(weights)
    args += weights
    whole = pl.BlockSpec((2 * half, width), lambda t: (0, 0))
    if acc is not None:
        specs.append(whole)
        args.append(acc)
    return pl.pallas_call(
        kernel,
        grid=(steps,),
        in_specs=specs,
        out_specs=whole,
        out_shape=jax.ShapeDtypeStruct((2 * half, width), F32),
        cost_estimate=pl.CostEstimate(
            flops=4 * half * depth * width * len(weights),
            bytes_accessed=6_000_000 * len(weights),
            transcendentals=0,
        ),
        compiler_params=vmem(20),
    )(*args)


def rows_of(q, k, piece):
    part = piece // 4
    sy = lax.rem(k + 4 - q[0], 4) * piece
    return [(pl.multiple_of(sy + lax.rem(i + 4 - q[4], 4) * part, part), part) for i in range(4)]


def last_kernel(q, own, oth, dig_own, dig_oth, w, acc, *rest):
    *e_outs, st_out, total = rest
    t = pl.program_id(0)

    @pl.when(t == 0)
    def _():
        total[...] = acc[...]

    add_products(total, ((own, oth),), (w,))

    @pl.when(t == pl.num_programs(0) - 1)
    def _():
        half = own.shape[0]
        piece = half // 4
        per = 4 // len(e_outs)
        for k in range(4):
            for sc in range(2):
                near = q[5] == sc
                spots = rows_of(q, k, piece)
                first = jnp.where(near, 0, half)
                logits = jnp.concatenate([total[pl.ds(first + a, b), :] for a, b in spots])
                digits = jnp.where(
                    near,
                    jnp.concatenate([dig_own[pl.ds(a, b), :] for a, b in spots]).astype(F32),
                    jnp.concatenate([dig_oth[pl.ds(a, b), :] for a, b in spots]).astype(F32),
                )
                target = (
                    digits[:, 0:1] * 65536.0 + digits[:, 1:2] * 256.0 + digits[:, 2:3]
                ).astype(jnp.int32) - q[3]
                top = jnp.max(logits, axis=1, keepdims=True)
                expo = jnp.exp(logits - top)
                col = lax.broadcasted_iota(jnp.int32, logits.shape, 1)
                mine = col < q[1]
                count = jnp.sum(jnp.where(mine, expo, 0.0), axis=1, keepdims=True)
                hit = (col + q[2] == target) & mine
                at_target = jnp.sum(jnp.where(hit, logits, 0.0), axis=1, keepdims=True)
                to = (2 * (k % per) + sc) * piece
                e_outs[k // per][to : to + piece, :] = expo.astype(BF)
                lane = lax.broadcasted_iota(jnp.int32, (piece, LANES), 1)
                st_out[(2 * k + sc) * piece : (2 * k + sc + 1) * piece, :] = jnp.where(
                    lane == 0,
                    top,
                    jnp.where(
                        lane == 1, count, jnp.where(lane == 2, at_target, target.astype(F32))
                    ),
                )


def logits_last(q, own, oth, w, acc, step, chunks):
    depth, width = w.shape
    half = own.shape[0]
    steps = depth // step
    rows = 2 * half
    weight = pl.BlockSpec((step, width), lambda t, q: (t, 0))
    digits = pl.BlockSpec((half, LANES), lambda t, q: (0, 2 * depth // LANES))
    const = lambda s: pl.BlockSpec(s, lambda t, q: (0, 0))
    e_shape = (rows // chunks, width)
    return pl.pallas_call(
        last_kernel,
        grid_spec=pltpu.PrefetchScalarGridSpec(
            num_scalar_prefetch=1,
            grid=(steps,),
            in_specs=strips(half, step, steps)
            + [digits, digits, weight, const((rows, width))],
            out_specs=[const(e_shape)] * chunks + [const((rows, LANES))],
            scratch_shapes=[pltpu.VMEM((rows, width), F32)],
        ),
        out_shape=[jax.ShapeDtypeStruct(e_shape, BF)] * chunks
        + [jax.ShapeDtypeStruct((rows, LANES), F32)],
        cost_estimate=pl.CostEstimate(
            flops=8 * half * depth * width, bytes_accessed=14_000_000, transcendentals=0
        ),
        compiler_params=vmem(24),
        name="logits_last",
    )(q, own, oth, own, oth, w, acc)


def transpose_kernel(q, own, oth, out):
    piece = own.shape[0] // 4
    for k in range(4):
        spots = rows_of(q, k, piece)
        near, far = (
            jnp.concatenate([src[pl.ds(a, b), :] for a, b in spots]).astype(F32)
            for src in (own, oth)
        )
        for sc in range(2):
            to = (2 * k + sc) * piece
            block = jnp.where(q[5] == sc, near, far)
            out[:, to : to + piece] = block.T.astype(BF)


def transposed(q, own, oth, depth, block):
    half = own.shape[0]
    source = pl.BlockSpec((half, block), lambda t, q: (0, t))
    return pl.pallas_call(
        transpose_kernel,
        grid_spec=pltpu.PrefetchScalarGridSpec(
            num_scalar_prefetch=1,
            grid=(depth // block,),
            in_specs=[source, source],
            out_specs=pl.BlockSpec((block, 2 * half), lambda t, q: (t, 0)),
        ),
        out_shape=jax.ShapeDtypeStruct((depth, 2 * half), BF),
        cost_estimate=pl.CostEstimate(
            flops=4_000_000, bytes_accessed=5_000_000, transcendentals=0
        ),
        compiler_params=vmem(10),
        name="transposed",
    )(q, own, oth)


def grad_kernel(offs, own, nxt, top, low, prev, coef, stats, head, grads, keep, send):
    rows = own.shape[0]
    half = rows // 2

    @pl.when(pl.program_id(0) == 0)
    def _():
        for h in range(2):
            at = pl.ds(h * half, half)
            across = (top, low)[h][...]
            target = stats[at, 3:4].astype(jnp.int32)
            for s, e in enumerate((own[at, :], nxt[at, :], across, prev[at, :])):
                start = pl.multiple_of(offs[s] * LANES, LANES)
                col = lax.broadcasted_iota(jnp.int32, e.shape, 1)
                prob = e.astype(F32) * coef[at, s : s + 1]
                grad = jnp.where(col == target - start, coef[at, 4:5], prob)
                grads[at, pl.ds(start, e.shape[1])] = grad.astype(BF)

    part = lax.dot_general(
        grads[...], head[...], (((1,), (1,)), ((), ())), preferred_element_type=F32
    )
    piece = rows // 4
    for i in range(2):
        for r in range(0, piece, 8):
            plane = lax.rem(r // 8 % 4 + 4 - offs[4], 4)
            level = lax.rem(r // 32 + 4 - offs[5], 4)
            to = pl.ds(pl.multiple_of(i * piece + level * 32 + plane * 8, 8), 8)
            at = 2 * i * piece + r
            north, south = part[at : at + 8], part[at + piece : at + piece + 8]
            keep[to, :] = jnp.where(offs[6] == 0, north, south)
            send[to, :] = jnp.where(offs[6] == 0, south, north)


def grads_of(offs, es, coef, stats, head_t, chunk, block):
    own, _, _, _, _ = es
    rows, _ = own.shape
    depth, width_dev = head_t.shape
    const = lambda a, i=0: pl.BlockSpec(a, lambda t, o: (i, 0))
    strip = pl.BlockSpec((rows // 2, block), lambda t, o: (0, t))
    return pl.pallas_call(
        grad_kernel,
        grid_spec=pltpu.PrefetchScalarGridSpec(
            num_scalar_prefetch=1,
            grid=(depth // block,),
            in_specs=[const(e.shape) for e in es]
            + [const((rows, LANES), chunk), const((rows, LANES), chunk)]
            + [pl.BlockSpec((block, width_dev), lambda t, o: (t, 0))],
            out_specs=[const((rows, width_dev)), strip, strip],
        ),
        out_shape=[
            jax.ShapeDtypeStruct((rows, width_dev), BF),
            jax.ShapeDtypeStruct((rows // 2, depth), F32),
            jax.ShapeDtypeStruct((rows // 2, depth), F32),
        ],
        cost_estimate=pl.CostEstimate(
            flops=2 * rows * width_dev * depth, bytes_accessed=15_000_000, transcendentals=0
        ),
        compiler_params=vmem(26),
        name="grads",
    )(offs, *es, coef, stats, head_t)


def head_kernel(ht, *refs):
    grads, out = refs[:-1], refs[-1]
    total = None
    at = 0
    for g in grads:
        depth = g.shape[0]
        part = jnp.dot(ht[:, at : at + depth], g[...], preferred_element_type=F32)
        total = part if total is None else total + part
        at += depth
    out[...] = total.astype(BF)


def head_grad_of(ht, grads, block):
    rows, depth = ht.shape
    width = grads[0].shape[1]
    return pl.pallas_call(
        head_kernel,
        grid=(pl.cdiv(width, block),),
        in_specs=[pl.BlockSpec((rows, depth), lambda i: (0, 0))]
        + [pl.BlockSpec((g.shape[0], block), lambda i: (0, i)) for g in grads],
        out_specs=pl.BlockSpec((rows, block), lambda i: (0, i)),
        out_shape=jax.ShapeDtypeStruct((rows, width), BF),
        cost_estimate=pl.CostEstimate(
            flops=2 * rows * depth * width, bytes_accessed=16_000_000, transcendentals=0
        ),
        compiler_params=vmem(26),
        name="head_grad",
    )(ht, *grads)


def everywhere(a, order=(1, 3, 2)):
    got = {0: a}
    for s in order:
        got[s] = shift_x(a, -s)
    return [got[s] for s in range(4)]


def around(a, axis):
    got = {}
    for s in (1, 3, 2):
        got[s] = shift_v(a, -s, 0, 0) if axis == 0 else shift_v(a, 0, -s, 0)
    return [a] + [got[s] for s in (1, 2, 3)]


def over_cores(keep, send):
    got = shift_v(send, 0, 0, 1)
    return keep + got


def scatter_tokens(mine):
    depth = mine.shape[-1]
    mine = mine.reshape(-1, 4, 4, 8, depth)
    parts = []
    for j in (1, 3, 2):
        parts.append(shift_v(mine[:, :, j], j, 0, 0))
    mine = mine[:, :, 0] + parts[0] + parts[1] + parts[2]
    parts = []
    for j in (1, 3, 2):
        parts.append(shift_v(mine[:, j], 0, j, 0))
    mine = mine[:, 0] + parts[0] + parts[1] + parts[2]
    return mine.reshape(-1, depth)


def step(hidden, head_t, targets, token_ids, embed_cot):
    x, v = lax.axis_index("dp"), lax.axis_index("vocab")
    y, z, c = v // 8, (v // 2) % 4, v % 2
    depth, width_dev = head_t.shape
    group = hidden.shape[0]
    planes = lax.axis_size("dp")
    tokens = group * planes
    tiles_dev = width_dev // LANES
    tiles = -(-tiles_dev // planes)
    width = tiles * LANES
    base = v * width_dev
    chunks = 2
    rows = tokens // chunks

    def off(q):
        return jnp.minimum(q * tiles, tiles_dev - tiles)

    slot_plane = [(x + s) % planes for s in range(planes)]
    offs = jnp.stack([off(q) for q in slot_plane]).astype(jnp.int32)

    row = 32 * (v % 8) + 8 * (v // 8)
    tgt = lax.dynamic_slice_in_dim(targets, row, 8)[:, None]
    ids = token_ids.reshape(8, group // 8)

    def base_256(a):
        return [a // 65536, (a // 256) % 256, a % 256]

    digits = jnp.concatenate(
        [*base_256(tgt), jnp.zeros((8, LANES - 3 - 3 * ids.shape[1]), jnp.int32), *base_256(ids)],
        axis=1,
    ).astype(BF)
    rows_mine = lax.dynamic_slice_in_dim(hidden, row, 8, axis=0)
    row_parts = everywhere(jnp.concatenate([rows_mine, digits], axis=1))
    moved = {}
    for s in (1, 3, 2):
        (block,) = pack(head_t, offs[s : s + 1], tiles)
        moved[s] = shift_x(block, s)
    w_prev, w_across, w_next = moved[1], moved[2], moved[3]

    at = jnp.stack(slot_plane).astype(jnp.int32)
    left, right = assemble(at, row_parts, depth)
    left = left.reshape(32, -1)
    right = right.reshape(32, -1)
    left = jnp.concatenate(around(left, 0))
    right = jnp.concatenate(around(right, 1))
    left = jnp.stack([a.reshape(4, 32, -1) for a in around(left, 1)], axis=1)
    left = left.reshape(tokens // 2, -1)
    right = jnp.concatenate(around(right, 0))
    left_oth = shift_v(left, 0, 0, 1)
    right_oth = shift_v(right, 0, 0, 1)

    bound = 2 * group // lax.axis_size("vocab")
    slot_numbers = jnp.arange(bound, dtype=jnp.int32)

    def compact(ids):
        inside = (ids >= base) & (ids < base + width_dev)
        rank = jnp.cumsum(inside.astype(jnp.int32)) - 1
        return (rank[None, :] == slot_numbers[:, None]) & inside[None, :]

    id_digits = jnp.stack([p[:, planes * depth + LANES - 3 * ids.shape[1] :] for p in row_parts])
    d = id_digits.astype(jnp.int32).reshape(planes, 8, 3, ids.shape[1])
    group_ids = (d[:, :, 0] * 65536 + d[:, :, 1] * 256 + d[:, :, 2]).reshape(planes, group)
    matches = jax.vmap(compact)(group_ids)
    picked = jnp.dot(
        matches[0].astype(BF), embed_cot, preferred_element_type=F32
    ).astype(BF)

    def cot_for(s):
        return lax.dynamic_slice_in_dim(picked, slot_plane[s] * depth, depth, axis=1)

    received = [cot_for(0)]
    for s in (1, 2, 3):
        received.append(shift_x(cot_for(planes - s), -s))
    received = jnp.concatenate(received)
    slot_ids = jnp.sum(jnp.where(matches, group_ids[:, None, :] - base, 0), axis=-1)
    slot_ids = jnp.where(jnp.any(matches, axis=-1), slot_ids, -1).reshape(-1)
    local_columns = jnp.arange(width_dev, dtype=jnp.int32)[None, :]
    slot_hot = (local_columns == slot_ids[:, None]).astype(BF)
    embed_grad = lax.dot_general(
        received, slot_hot, (((0,), (0,)), ((), ())), preferred_element_type=F32
    ).astype(BF)

    (own_w,) = pack(head_t, offs[:1], tiles)
    valid = jnp.where(x == planes - 2, (tiles_dev - tiles - off(x)) * LANES, width)
    q = jnp.stack([y, valid, off(x) * LANES, base, z, c]).astype(jnp.int32)
    ht = transposed(q, left, left_oth, depth, 256)
    left, ht = lax.optimization_barrier((left, ht))
    acc = partial_logits(
        first_kernel, [(left, left_oth, 0), (left, left_oth, 1)], [own_w, w_prev], None, 256
    )
    acc = partial_logits(mid_kernel, [(right, right_oth, 0)], [w_next], acc, 256)
    *expo, stats = logits_last(q, right, right_oth, w_across, acc, 256, chunks)

    es = []
    for e in expo:
        prev = shift_x(e, 1)
        next_ = shift_x(e, -1)
        es.append((e, next_, prev))

    st = stats[:, :3].T.reshape(3, tokens // LANES, LANES)
    both = jnp.broadcast_to(st, (lax.axis_size("vocab"), *st.shape))
    both = lax.all_to_all(both, "vocab", split_axis=0, concat_axis=0, tiled=True)

    def joined(tops, sums, hits):
        top = jnp.max(tops, axis=0)
        return top, jnp.sum(sums * jnp.exp(tops - top), axis=0), jnp.sum(hits, axis=0)

    plane_stats = jnp.stack([*joined(both[:, 0], both[:, 1], both[:, 2]), st[0]])
    parts = jnp.stack(everywhere(plane_stats))
    row_max, row_sum, hit = joined(parts[:, 0], parts[:, 1], parts[:, 2])
    scale = jnp.exp(parts[:, 3] - row_max) / row_sum
    at_target = jnp.exp(hit - row_max) / row_sum - 1.0
    coef = jnp.concatenate([scale, at_target[None]]).reshape(5, tokens).T
    coef = jnp.pad(coef, ((0, 0), (0, LANES - 5)))

    offs_y = jnp.concatenate([offs, jnp.stack([y, z, c]).astype(jnp.int32)])
    grads, pieces = [], []
    mine = None
    for i in range(chunks):
        e, next_, prev = es[i]
        half = rows // 2
        top = shift_x(prev[:half], 1)
        low = shift_x(next_[half:], -1)
        if mine is not None:
            coef, mine = lax.optimization_barrier((coef, mine))
            pieces.append(scatter_tokens(mine))
        g, keep, send = grads_of(offs_y, (e, next_, top, low, prev), coef, stats, head_t, i, 256)
        grads.append(g)
        mine = over_cores(keep, send)
    pieces.append(scatter_tokens(mine))
    hidden_grad = jnp.concatenate(pieces).astype(BF)
    head_grad = head_grad_of(ht, grads, 512)
    return (head_grad, embed_grad, hidden_grad)


def solution(mesh):
    placed = (P("dp", None), P("dp", "vocab"), P("dp"), P("dp"), P("dp", None))
    return jax.shard_map(
        step,
        mesh=mesh,
        in_specs=placed,
        out_specs=(P("dp", "vocab"), P("dp", "vocab"), P("vocab", "dp")),
        check_vma=False,
    )
```

```python
import jax
import jax.numpy as jnp
from jax import lax
from jax.experimental import pallas as pl
from jax.experimental.pallas import tpu as pltpu
from jax.sharding import PartitionSpec as P


LANES = 128
STEP = 640
BF = jnp.bfloat16
F32 = jnp.float32


def shift_x(a, s):
    n = lax.axis_size("dp")
    return lax.ppermute(a, "dp", [(i, (i + s) % n) for i in range(n)])


def vocab_perm(dy, dz, dc):
    pairs = []
    for v in range(32):
        y, z, c = v // 8, (v // 2) % 4, v % 2
        pairs.append((v, ((y + dy) % 4) * 8 + ((z + dz) % 4) * 2 + (c + dc) % 2))
    return pairs


def shift_v(a, dy, dz, dc):
    return lax.ppermute(a, "vocab", vocab_perm(dy, dz, dc))


def vmem(mib):
    return pltpu.CompilerParams(vmem_limit_bytes=mib * 2**20)


def pack_kernel(offs, src, dst, sem):
    start = pl.multiple_of(offs[0] * LANES, LANES)
    copy = pltpu.make_async_copy(src.at[:, pl.ds(start, dst.shape[1])], dst, sem)
    copy.start()
    copy.wait()


def pack(head_t, offs, tiles):
    shape = (head_t.shape[0], tiles * LANES)
    return pl.pallas_call(
        pack_kernel,
        grid_spec=pltpu.PrefetchScalarGridSpec(
            num_scalar_prefetch=1,
            grid=(1,),
            in_specs=[pl.BlockSpec(memory_space=pltpu.HBM)],
            out_specs=pl.BlockSpec(shape, lambda i, o: (0, 0)),
            scratch_shapes=[pltpu.SemaphoreType.DMA],
        ),
        out_shape=jax.ShapeDtypeStruct(shape, BF),
        compiler_params=vmem(60),
        name="pack",
    )(offs, head_t)


def assemble_kernel(at, p0, p1, p2, p3, left, right):
    depth = left.shape[-1] // 2
    for s, p in enumerate((p0, p1, p2, p3)):
        j = at[s]
        for dst, first, second in ((left, 0, 3), (right, 1, 2)):
            for i, slot in enumerate((first, second)):
                start = pl.multiple_of(at[slot] * depth, depth)
                dst[j, :, i * depth : (i + 1) * depth] = p[:, pl.ds(start, depth)]
        right[j, :, 2 * depth :] = p[:, 4 * depth :]


def assemble(at, parts, depth):
    rows = parts[0].shape[0]
    whole = lambda shape: pl.BlockSpec(shape, lambda i, at: (0,) * len(shape))
    shapes = [(4, rows, 2 * depth), (4, rows, 2 * depth + LANES)]
    return pl.pallas_call(
        assemble_kernel,
        grid_spec=pltpu.PrefetchScalarGridSpec(
            num_scalar_prefetch=1,
            grid=(1,),
            in_specs=[whole(parts[0].shape)] * 4,
            out_specs=[whole(s) for s in shapes],
        ),
        out_shape=[jax.ShapeDtypeStruct(s, BF) for s in shapes],
        compiler_params=vmem(8),
        name="assemble",
    )(at, *parts)


def add_products(total, pairs, weights):
    half = pairs[0][0].shape[0]
    for i in range(2):
        part = None
        for pair, w in zip(pairs, weights):
            new = jnp.dot(pair[i][...], w[...], preferred_element_type=F32)
            part = new if part is None else part + new
        total[i * half : (i + 1) * half, :] += part


def first_kernel(own1, oth1, own2, oth2, w1, w2, out):
    @pl.when(pl.program_id(0) == 0)
    def _():
        out[...] = jnp.zeros_like(out)

    add_products(out, ((own1, oth1), (own2, oth2)), (w1, w2))


def mid_kernel(own, oth, w, acc, out):
    @pl.when(pl.program_id(0) == 0)
    def _():
        out[...] = acc[...]

    add_products(out, ((own, oth),), (w,))


def strips(half, step, start):
    spec = lambda: pl.BlockSpec((half, step), lambda t, *q: (0, t + start))
    return [spec(), spec()]


def partial_logits(kernel, sources, weights, acc, step):
    depth, width = weights[0].shape
    steps = depth // step
    half = sources[0][0].shape[0]
    specs, args = [], []
    for own, oth, start in sources:
        specs += strips(half, step, start * steps)
        args += [own, oth]
    specs += [pl.BlockSpec((step, width), lambda t: (t, 0))] * len(weights)
    args += weights
    whole = pl.BlockSpec((2 * half, width), lambda t: (0, 0))
    if acc is not None:
        specs.append(whole)
        args.append(acc)
    return pl.pallas_call(
        kernel,
        grid=(steps,),
        in_specs=specs,
        out_specs=whole,
        out_shape=jax.ShapeDtypeStruct((2 * half, width), F32),
        cost_estimate=pl.CostEstimate(
            flops=4 * half * depth * width * len(weights),
            bytes_accessed=6_000_000 * len(weights),
            transcendentals=0,
        ),
        compiler_params=vmem(20),
    )(*args)


def rows_of(q, k, piece):
    part = piece // 4
    sy = lax.rem(k + 4 - q[0], 4) * piece
    return [(pl.multiple_of(sy + lax.rem(i + 4 - q[4], 4) * part, part), part) for i in range(4)]


def last_kernel(q, own, oth, dig_own, dig_oth, w, acc, *rest):
    *e_outs, st_out, total = rest
    t = pl.program_id(0)

    @pl.when(t == 0)
    def _():
        total[...] = acc[...]

    add_products(total, ((own, oth),), (w,))

    @pl.when(t == pl.num_programs(0) - 1)
    def _():
        half = own.shape[0]
        piece = half // 4
        per = 4 // len(e_outs)
        for k in range(4):
            for sc in range(2):
                near = q[5] == sc
                spots = rows_of(q, k, piece)
                first = jnp.where(near, 0, half)
                logits = jnp.concatenate([total[pl.ds(first + a, b), :] for a, b in spots])
                digits = jnp.where(
                    near,
                    jnp.concatenate([dig_own[pl.ds(a, b), :] for a, b in spots]).astype(F32),
                    jnp.concatenate([dig_oth[pl.ds(a, b), :] for a, b in spots]).astype(F32),
                )
                target = (
                    digits[:, 0:1] * 65536.0 + digits[:, 1:2] * 256.0 + digits[:, 2:3]
                ).astype(jnp.int32) - q[3]
                top = jnp.max(logits, axis=1, keepdims=True)
                expo = jnp.exp(logits - top)
                col = lax.broadcasted_iota(jnp.int32, logits.shape, 1)
                mine = col < q[1]
                count = jnp.sum(jnp.where(mine, expo, 0.0), axis=1, keepdims=True)
                hit = (col + q[2] == target) & mine
                at_target = jnp.sum(jnp.where(hit, logits, 0.0), axis=1, keepdims=True)
                to = (2 * (k % per) + sc) * piece
                e_outs[k // per][to : to + piece, :] = expo.astype(BF)
                lane = lax.broadcasted_iota(jnp.int32, (piece, LANES), 1)
                st_out[(2 * k + sc) * piece : (2 * k + sc + 1) * piece, :] = jnp.where(
                    lane == 0,
                    top,
                    jnp.where(
                        lane == 1, count, jnp.where(lane == 2, at_target, target.astype(F32))
                    ),
                )


def logits_last(q, own, oth, w, acc, step, chunks):
    depth, width = w.shape
    half = own.shape[0]
    steps = depth // step
    rows = 2 * half
    weight = pl.BlockSpec((step, width), lambda t, q: (t, 0))
    digits = pl.BlockSpec((half, LANES), lambda t, q: (0, 2 * depth // LANES))
    const = lambda s: pl.BlockSpec(s, lambda t, q: (0, 0))
    e_shape = (rows // chunks, width)
    return pl.pallas_call(
        last_kernel,
        grid_spec=pltpu.PrefetchScalarGridSpec(
            num_scalar_prefetch=1,
            grid=(steps,),
            in_specs=strips(half, step, steps)
            + [digits, digits, weight, const((rows, width))],
            out_specs=[const(e_shape)] * chunks + [const((rows, LANES))],
            scratch_shapes=[pltpu.VMEM((rows, width), F32)],
        ),
        out_shape=[jax.ShapeDtypeStruct(e_shape, BF)] * chunks
        + [jax.ShapeDtypeStruct((rows, LANES), F32)],
        cost_estimate=pl.CostEstimate(
            flops=8 * half * depth * width, bytes_accessed=14_000_000, transcendentals=0
        ),
        compiler_params=vmem(24),
        name="logits_last",
    )(q, own, oth, own, oth, w, acc)


def transpose_kernel(q, own, oth, out):
    piece = own.shape[0] // 4
    for k in range(4):
        spots = rows_of(q, k, piece)
        near, far = (
            jnp.concatenate([src[pl.ds(a, b), :] for a, b in spots]).astype(F32)
            for src in (own, oth)
        )
        for sc in range(2):
            to = (2 * k + sc) * piece
            block = jnp.where(q[5] == sc, near, far)
            out[:, to : to + piece] = block.T.astype(BF)


def transposed(q, own, oth, depth, block):
    half = own.shape[0]
    source = pl.BlockSpec((half, block), lambda t, q: (0, t))
    return pl.pallas_call(
        transpose_kernel,
        grid_spec=pltpu.PrefetchScalarGridSpec(
            num_scalar_prefetch=1,
            grid=(depth // block,),
            in_specs=[source, source],
            out_specs=pl.BlockSpec((block, 2 * half), lambda t, q: (t, 0)),
        ),
        out_shape=jax.ShapeDtypeStruct((depth, 2 * half), BF),
        cost_estimate=pl.CostEstimate(
            flops=4_000_000, bytes_accessed=5_000_000, transcendentals=0
        ),
        compiler_params=vmem(10),
        name="transposed",
    )(q, own, oth)


def grad_kernel(offs, own, nxt, top, low, prev, coef, stats, head, grads, keep, send):
    rows = own.shape[0]
    half = rows // 2

    @pl.when(pl.program_id(0) == 0)
    def _():
        for h in range(2):
            at = pl.ds(h * half, half)
            across = (top, low)[h][...]
            target = stats[at, 3:4].astype(jnp.int32)
            for s, e in enumerate((own[at, :], nxt[at, :], across, prev[at, :])):
                start = pl.multiple_of(offs[s] * LANES, LANES)
                col = lax.broadcasted_iota(jnp.int32, e.shape, 1)
                prob = e.astype(F32) * coef[at, s : s + 1]
                grad = jnp.where(col == target - start, coef[at, 4:5], prob)
                grads[at, pl.ds(start, e.shape[1])] = grad.astype(BF)

    part = lax.dot_general(
        grads[...], head[...], (((1,), (1,)), ((), ())), preferred_element_type=F32
    )
    piece = rows // 4
    for i in range(2):
        for r in range(0, piece, 8):
            plane = lax.rem(r // 8 % 4 + 4 - offs[4], 4)
            level = lax.rem(r // 32 + 4 - offs[5], 4)
            to = pl.ds(pl.multiple_of(i * piece + level * 32 + plane * 8, 8), 8)
            at = 2 * i * piece + r
            north, south = part[at : at + 8], part[at + piece : at + piece + 8]
            keep[to, :] = jnp.where(offs[6] == 0, north, south)
            send[to, :] = jnp.where(offs[6] == 0, south, north)


def grads_of(offs, es, coef, stats, head_t, chunk, block):
    own, _, _, _, _ = es
    rows, _ = own.shape
    depth, width_dev = head_t.shape
    const = lambda a, i=0: pl.BlockSpec(a, lambda t, o: (i, 0))
    strip = pl.BlockSpec((rows // 2, block), lambda t, o: (0, t))
    return pl.pallas_call(
        grad_kernel,
        grid_spec=pltpu.PrefetchScalarGridSpec(
            num_scalar_prefetch=1,
            grid=(depth // block,),
            in_specs=[const(e.shape) for e in es]
            + [const((rows, LANES), chunk), const((rows, LANES), chunk)]
            + [pl.BlockSpec((block, width_dev), lambda t, o: (t, 0))],
            out_specs=[const((rows, width_dev)), strip, strip],
        ),
        out_shape=[
            jax.ShapeDtypeStruct((rows, width_dev), BF),
            jax.ShapeDtypeStruct((rows // 2, depth), F32),
            jax.ShapeDtypeStruct((rows // 2, depth), F32),
        ],
        cost_estimate=pl.CostEstimate(
            flops=2 * rows * width_dev * depth, bytes_accessed=15_000_000, transcendentals=0
        ),
        compiler_params=vmem(26),
        name="grads",
    )(offs, *es, coef, stats, head_t)


def head_kernel(ht, *refs):
    grads, out = refs[:-1], refs[-1]
    total = None
    at = 0
    for g in grads:
        depth = g.shape[0]
        part = jnp.dot(ht[:, at : at + depth], g[...], preferred_element_type=F32)
        total = part if total is None else total + part
        at += depth
    out[...] = total.astype(BF)


def head_grad_of(ht, grads, block):
    rows, depth = ht.shape
    width = grads[0].shape[1]
    return pl.pallas_call(
        head_kernel,
        grid=(pl.cdiv(width, block),),
        in_specs=[pl.BlockSpec((rows, depth), lambda i: (0, 0))]
        + [pl.BlockSpec((g.shape[0], block), lambda i: (0, i)) for g in grads],
        out_specs=pl.BlockSpec((rows, block), lambda i: (0, i)),
        out_shape=jax.ShapeDtypeStruct((rows, width), BF),
        cost_estimate=pl.CostEstimate(
            flops=2 * rows * depth * width, bytes_accessed=16_000_000, transcendentals=0
        ),
        compiler_params=vmem(26),
        name="head_grad",
    )(ht, *grads)


def everywhere(a, order=(1, 3, 2)):
    got = {0: a}
    for s in order:
        got[s] = shift_x(a, -s)
    return [got[s] for s in range(4)]


def around(a, axis):
    got = {}
    for s in (1, 3, 2):
        got[s] = shift_v(a, -s, 0, 0) if axis == 0 else shift_v(a, 0, -s, 0)
    return [a] + [got[s] for s in (1, 2, 3)]


def over_cores(keep, send):
    got = shift_v(send, 0, 0, 1)
    return keep + got


def scatter_tokens(mine):
    depth = mine.shape[-1]
    mine = mine.reshape(-1, 4, 4, 8, depth)
    parts = []
    for j in (1, 3, 2):
        parts.append(shift_v(mine[:, :, j], j, 0, 0))
    mine = mine[:, :, 0] + parts[0] + parts[1] + parts[2]
    parts = []
    for j in (1, 3, 2):
        parts.append(shift_v(mine[:, j], 0, j, 0))
    mine = mine[:, 0] + parts[0] + parts[1] + parts[2]
    return mine.reshape(-1, depth)


def step(hidden, head_t, targets, token_ids, embed_cot):
    x, v = lax.axis_index("dp"), lax.axis_index("vocab")
    y, z, c = v // 8, (v // 2) % 4, v % 2
    depth, width_dev = head_t.shape
    group = hidden.shape[0]
    planes = lax.axis_size("dp")
    tokens = group * planes
    tiles_dev = width_dev // LANES
    tiles = -(-tiles_dev // planes)
    width = tiles * LANES
    base = v * width_dev
    chunks = 2
    rows = tokens // chunks

    def off(q):
        return jnp.minimum(q * tiles, tiles_dev - tiles)

    slot_plane = [(x + s) % planes for s in range(planes)]
    offs = jnp.stack([off(q) for q in slot_plane]).astype(jnp.int32)

    row = 32 * (v % 8) + 8 * (v // 8)
    tgt = lax.dynamic_slice_in_dim(targets, row, 8)[:, None]
    ids = token_ids.reshape(8, group // 8)

    def base_256(a):
        return [a >> 16, (a >> 8) & 255, a & 255]

    digits = jnp.concatenate(
        [*base_256(tgt), jnp.zeros((8, LANES - 3 - 3 * ids.shape[1]), jnp.int32), *base_256(ids)],
        axis=1,
    ).astype(BF)
    rows_mine = lax.dynamic_slice_in_dim(hidden, row, 8, axis=0)
    row_parts = everywhere(jnp.concatenate([rows_mine, digits], axis=1))
    moved = {}
    for s in (1, 3, 2):
        block = pack(head_t, offs[s : s + 1], tiles)
        moved[s] = shift_x(block, s)
    w_prev, w_across, w_next = moved[1], moved[2], moved[3]

    at = jnp.stack(slot_plane).astype(jnp.int32)
    left, right = assemble(at, row_parts, depth)
    left = left.reshape(32, -1)
    right = right.reshape(32, -1)
    left = jnp.concatenate(around(left, 0))
    right = jnp.concatenate(around(right, 1))
    left = jnp.stack([a.reshape(4, 32, -1) for a in around(left, 1)], axis=1)
    left = left.reshape(tokens // 2, -1)
    right = jnp.concatenate(around(right, 0))
    left_oth = shift_v(left, 0, 0, 1)
    right_oth = shift_v(right, 0, 0, 1)

    bound = 2 * group // lax.axis_size("vocab")
    slot_numbers = jnp.arange(bound, dtype=jnp.int32)

    def compact(ids):
        inside = (ids >= base) & (ids < base + width_dev)
        rank = jnp.cumsum(inside.astype(jnp.int32)) - 1
        return (rank[None, :] == slot_numbers[:, None]) & inside[None, :]

    id_digits = jnp.stack([p[:, planes * depth + LANES - 3 * ids.shape[1] :] for p in row_parts])
    d = id_digits.astype(jnp.int32).reshape(planes, 8, 3, ids.shape[1])
    group_ids = (d[:, :, 0] * 65536 + d[:, :, 1] * 256 + d[:, :, 2]).reshape(planes, group)
    matches = jax.vmap(compact)(group_ids)
    picked = jnp.dot(
        matches[0].astype(BF), embed_cot, preferred_element_type=F32
    ).astype(BF)

    def cot_for(s):
        return lax.dynamic_slice_in_dim(picked, slot_plane[s] * depth, depth, axis=1)

    received = [cot_for(0)]
    for s in (1, 2, 3):
        received.append(shift_x(cot_for(planes - s), -s))
    received = jnp.concatenate(received)
    slot_ids = jnp.sum(jnp.where(matches, group_ids[:, None, :] - base, 0), axis=-1)
    slot_ids = jnp.where(jnp.any(matches, axis=-1), slot_ids, -1).reshape(-1)
    local_columns = jnp.arange(width_dev, dtype=jnp.int32)[None, :]
    slot_hot = (local_columns == slot_ids[:, None]).astype(BF)
    embed_grad = lax.dot_general(
        received, slot_hot, (((0,), (0,)), ((), ())), preferred_element_type=F32
    ).astype(BF)

    own_w = pack(head_t, offs[:1], tiles)
    valid = jnp.where(x == planes - 2, (tiles_dev - tiles - off(x)) * LANES, width)
    q = jnp.stack([y, valid, off(x) * LANES, base, z, c]).astype(jnp.int32)
    ht = transposed(q, left, left_oth, depth, 256)
    acc = partial_logits(
        first_kernel, [(left, left_oth, 0), (left, left_oth, 1)], [own_w, w_prev], None, STEP
    )
    acc = partial_logits(mid_kernel, [(right, right_oth, 0)], [w_next], acc, STEP)
    *expo, stats = logits_last(q, right, right_oth, w_across, acc, depth, chunks)

    es = []
    for e in expo:
        prev = shift_x(e, 1)
        next_ = shift_x(e, -1)
        es.append((e, next_, prev))

    st = stats[:, :3].T.reshape(3, tokens // LANES, LANES)
    both = jnp.broadcast_to(st, (lax.axis_size("vocab"), *st.shape))
    both = lax.all_to_all(both, "vocab", split_axis=0, concat_axis=0, tiled=True)

    def joined(tops, sums, hits):
        top = jnp.max(tops, axis=0)
        return top, jnp.sum(sums * jnp.exp(tops - top), axis=0), jnp.sum(hits, axis=0)

    plane_stats = jnp.stack([*joined(both[:, 0], both[:, 1], both[:, 2]), st[0]])
    parts = jnp.stack(everywhere(plane_stats))
    row_max, row_sum, hit = joined(parts[:, 0], parts[:, 1], parts[:, 2])
    scale = jnp.exp(parts[:, 3] - row_max) / row_sum
    at_target = jnp.exp(hit - row_max) / row_sum - 1.0
    coef = jnp.concatenate([scale, at_target[None]]).reshape(5, tokens).T
    coef = jnp.pad(coef, ((0, 0), (0, LANES - 5)))

    offs_y = jnp.concatenate([offs, jnp.stack([y, z, c]).astype(jnp.int32)])
    grads, pieces = [], []
    mine = None
    for i in range(chunks):
        e, next_, prev = es[i]
        half = rows // 2
        top = shift_x(prev[:half], 1)
        low = shift_x(next_[half:], -1)
        if mine is not None:
            coef, mine = lax.optimization_barrier((coef, mine))
            pieces.append(scatter_tokens(mine))
        g, keep, send = grads_of(offs_y, (e, next_, top, low, prev), coef, stats, head_t, i, 256)
        grads.append(g)
        mine = over_cores(keep, send)
    pieces.append(scatter_tokens(mine))
    hidden_grad = jnp.concatenate(pieces).astype(BF)
    head_grad = head_grad_of(ht, grads, 512)
    return (head_grad, embed_grad, hidden_grad)


def solution(mesh):
    placed = (P("dp", None), P("dp", "vocab"), P("dp"), P("dp"), P("dp", None))
    return jax.shard_map(
        step,
        mesh=mesh,
        in_specs=placed,
        out_specs=(P("dp", "vocab"), P("dp", "vocab"), P("vocab", "dp")),
        check_vma=False,
    )
```
